32 devices in a mesh: group: 4 (over y, x), shard: 8 (over z, core).
Axes of the slice: x: 2, y: 2, z: 4, core: 2. Of those that a mesh axis runs over, the one named last changes fastest.
Arguments:
- grad_pooled: bfloat16 [4096, 512, 128], P(('group', 'shard')), may hold values from -6 to 6
- bag_rows: int32 [4096, 512, 8], P(('group', 'shard')), may hold values from 0 to 511
- bag_lengths: int32 [4096, 512], P(('group', 'shard')), may hold values from 1 to 8
- table_order: int32 [512], replicated, may hold values from 0 to 511, each once
- weights: bfloat16 [512, 512, 128], P('shard'), may hold values from -6 to 6
- accum: float32 [512, 512], P('shard'), may hold values from 0.1 to 10
Outputs:
- new_weights: bfloat16 [512, 512, 128], P('shard')
- new_accum: float32 [512, 512], P('shard')
The draws below stay inside these ranges and needn't reach their ends.
All inputs are finite; a program needn't handle non-finite values.
Results may differ from the reference program's by a relative error of at most 0.001.
Values may be sent and summed in bfloat16 or wider, within the bound.
A program may use at most 128 MiB of HBM per device.

```python
import math
import jax
import jax.numpy as jnp
from jax import lax

D = 128
TABLES = 512
ROWS = 512
BAG = 8
BATCH = 4096


def plant(values, own_key, smallest, high):
    longest = values.shape.index(max(values.shape))
    spots = []
    for shift in (0, 1):
        where = [jax.random.randint(jax.random.fold_in(own_key, axis), (), 0, length) for axis, length in enumerate(values.shape)]
        where[longest] = (where[longest] + shift) % values.shape[longest]
        spots.append(tuple(where))
    return values.at[spots[0]].set(smallest).at[spots[1]].set(high)


def steps_of(rng, dims, cuts, least, top_value):
    gain, own = 1.0, jax.random.fold_in(rng, 6)
    for axis_at, blocks in cuts:
        heights = jnp.exp(jax.random.uniform(jax.random.fold_in(own, axis_at), (blocks,), jnp.float32, least / len(cuts), top_value / len(cuts)))
        gain = gain * jnp.repeat(heights, dims[axis_at] // blocks).reshape([-1 if axis == axis_at else 1 for axis in range(len(dims))])
    return gain


def noise(own_key, shape, scale, reach, split=(), kind=jnp.bfloat16):
    level = steps_of(own_key, shape, split, -0.22, 0.18) if split else 1.0
    entries = jax.random.normal(own_key, shape, jnp.float32) * scale * level
    return jnp.minimum(jnp.maximum(entries, -reach), reach).astype(kind)


def setup_inputs(seed: int = 0) -> dict:
    seeds = jax.random.split(jax.random.key(seed), 7)
    grad_pooled = noise(seeds[0], (BATCH, TABLES, D), 1.0, 6.0, ((0, 32),))
    bag_rows = plant(jax.random.randint(seeds[1], (BATCH, TABLES, BAG), 0, ROWS), jax.random.fold_in(seeds[1], 1), 0, ROWS - 1).astype(jnp.int32)
    bag_lengths = plant(jax.random.randint(seeds[2], (BATCH, TABLES), 1, BAG + 1), jax.random.fold_in(seeds[2], 1), 1, BAG).astype(jnp.int32)
    table_order = jax.random.permutation(seeds[3], TABLES).astype(jnp.int32)
    weights = noise(seeds[4], (TABLES, ROWS, D), 1.0, 6.0, ((0, 8),))
    accum = jnp.clip(jnp.exp(math.log(10.0) - 4.6051702 * jax.random.uniform(seeds[5], (TABLES, ROWS), jnp.float32) ** steps_of(seeds[5], (TABLES, ROWS), ((0, 8),), -0.2, 0.2)), 0.1, 10.0)
    return dict(grad_pooled=grad_pooled, bag_rows=bag_rows, bag_lengths=bag_lengths, table_order=table_order, weights=weights, accum=accum)


LEARN_RATE = 0.5
EPSILON = 1e-06

def reference(grad_pooled, bag_rows, bag_lengths, table_order, weights, accum):
    pooled = jnp.take(grad_pooled, table_order, axis=1).astype(jnp.float32)
    places = jnp.arange(BAG, dtype=jnp.int32)
    live = places[None, None, :] < bag_lengths[:, :, None]
    row_ids = jnp.where(live, bag_rows, ROWS).astype(jnp.int32)
    row_ids = jnp.take(row_ids, table_order, axis=1)

    def one_table(member):
        values, chosen = member
        spread = jnp.broadcast_to(values[:, None, :], (values.shape[0], BAG, D)).reshape(-1, D)
        summed = jax.ops.segment_sum(spread, chosen.reshape(-1), num_segments=ROWS + 1)
        return summed[:ROWS]
    row_grad = lax.map(one_table, (jnp.swapaxes(pooled, 0, 1), jnp.swapaxes(row_ids, 0, 1)))
    new_accum = accum + lax.optimization_barrier(jnp.mean(row_grad * row_grad, axis=-1))
    step_size = LEARN_RATE / (jnp.sqrt(new_accum) + EPSILON)
    new_weights = (weights.astype(jnp.float32) - step_size[:, :, None] * row_grad).astype(jnp.bfloat16)
    return (new_weights, new_accum)
```

```python
import functools

import jax
import jax.numpy as jnp
from jax import lax
from jax.experimental import pallas as pl
from jax.experimental.pallas import tpu as pltpu
from jax.sharding import PartitionSpec as P

LEARN_RATE = 0.5
EPSILON = 1e-06
AXES = ("group", "shard")
TILE = 16
STEPS_AHEAD = 6
LEVELS = 32760.0
SMALLEST = 1e-30
MESH = pl.DeviceIdType.MESH


def arrange_kernel(order_ref, grad_ref, out_ref, flipped):
    tables = grad_ref.shape[1]

    def flip(step, carry):
        start = pl.multiple_of(step * TILE, TILE)
        block = grad_ref[:, pl.ds(start, TILE), :]
        flipped[pl.ds(start, TILE)] = jnp.swapaxes(block, 0, 1)
        return carry

    lax.fori_loop(0, tables // TILE, flip, 0)

    def place(step, carry):
        for k in range(8):
            at = step * 8 + k
            out_ref[at] = flipped[order_ref[at]]
        return carry

    lax.fori_loop(0, tables // 8, place, 0)


def arrange(grad_pooled, order):
    samples, tables, width = grad_pooled.shape
    return pl.pallas_call(
        arrange_kernel,
        grid_spec=pltpu.PrefetchScalarGridSpec(
            num_scalar_prefetch=1,
            grid=(samples // TILE,),
            in_specs=[pl.BlockSpec((TILE, tables, width), lambda b, order: (b, 0, 0))],
            out_specs=pl.BlockSpec((tables, TILE, width), lambda b, order: (0, b, 0)),
            scratch_shapes=[pltpu.VMEM((tables, TILE, width), grad_pooled.dtype)],
        ),
        out_shape=jax.ShapeDtypeStruct((tables, samples, width), grad_pooled.dtype),
        cost_estimate=pl.CostEstimate(
            flops=0, bytes_accessed=4 * grad_pooled.size, transcendentals=0
        ),
    )(order, grad_pooled)


def sum_rows(load_ids, load_values, sources, counts, acc, offset):
    row_count, wide = counts.shape
    bag, samples = load_ids(0).shape
    unroll = wide // samples
    place = lax.broadcasted_iota(jnp.int32, (TILE, samples), 0).astype(jnp.float32)
    places = [(place + float(r * TILE - offset)).astype(jnp.bfloat16) for r in range(row_count // TILE)]
    one = jnp.ones((TILE, samples), jnp.bfloat16)
    zero = jnp.zeros((TILE, samples), jnp.bfloat16)
    for turn in range(sources // unroll):
        for u in range(unroll):
            picks = load_ids(turn * unroll + u).astype(jnp.float32)
            spread = [
                jnp.broadcast_to(picks[j : j + 1], (TILE, samples)).astype(jnp.bfloat16)
                for j in range(bag)
            ]
            for r, here in enumerate(places):
                terms = [jnp.where(s == here, one, zero) for s in spread]
                while len(terms) > 1:
                    terms = [a + b for a, b in zip(terms[::2], terms[1::2])] + (
                        [terms[-1]] if len(terms) % 2 else []
                    )
                counts[r * TILE : (r + 1) * TILE, u * samples : (u + 1) * samples] = terms[0]
        values = load_values(turn * unroll, unroll)
        part = lax.dot_general(
            values, counts[...], (((0,), (1,)), ((), ())), preferred_element_type=jnp.float32
        )
        if turn == 0:
            acc[...] = part
        else:
            acc[...] += part


def exchange_kernel(
    cores, lines, offset,
    sends, ids, weights, accum, new_weights, new_accum,
    raw, raw_ids, counts, acc, parts, scales, got_parts, got_scales, own,
    held_weights, held_accum, made_weights, made_accum,
    raw_sent, raw_got, ids_sent, ids_got, local,
    parts_sent, parts_got, scales_sent, scales_got,
    weights_sent, weights_got, accum_sent, accum_got,
):
    steps, plane, batch = sends.shape[:3]
    groups = plane // cores
    rounds = steps // lines
    ahead = raw_sent.shape[0]
    bag, samples = ids.shape[-2:]
    width, row_count = acc.shape
    g = lax.axis_index("group")
    s = lax.axis_index("shard")
    z, c = s // cores, s % cores
    p = g * cores + c

    def in_plane(o):
        q = (p + o) % plane
        return q, (q // cores, z * cores + q % cores)

    def in_line(d):
        far = (z + 1 + d) % lines
        return far, (g, far * cores + c)

    barrier = pltpu.get_barrier_semaphore()
    for o in range(1, plane):
        pl.semaphore_signal(barrier, inc=1, device_id=in_plane(o)[1], device_id_type=MESH)
    for d in range(lines - 1):
        pl.semaphore_signal(barrier, inc=1, device_id=in_line(d)[1], device_id_type=MESH)

    locals_ = [
        pltpu.make_async_copy(sends.at[:, p], raw.at[:, p], local.at[0]),
        pltpu.make_async_copy(ids.at[p], raw_ids.at[p], local.at[1]),
        pltpu.make_async_copy(weights.at[g], held_weights, local.at[2]),
        pltpu.make_async_copy(accum.at[g], held_accum, local.at[3]),
    ]
    for copy in locals_:
        copy.start()
    pl.semaphore_wait(barrier, plane - 1 + lines - 1)

    for o in range(1, plane):
        q, device = in_plane(o)
        pltpu.make_async_remote_copy(
            src_ref=ids.at[q], dst_ref=raw_ids.at[p], send_sem=ids_sent, recv_sem=ids_got,
            device_id=device, device_id_type=MESH,
        ).start()

    def place_of(n):
        return in_line(n % lines)[0] * rounds + n // lines

    def send_raw(n):
        a = place_of(n)
        for o in range(1, plane):
            q, device = in_plane(o)
            pltpu.make_async_remote_copy(
                src_ref=sends.at[a, q], dst_ref=raw.at[a, p],
                send_sem=raw_sent.at[n % ahead], recv_sem=raw_got.at[a],
                device_id=device, device_id_type=MESH,
            ).start()

    def wait_bytes(ref, sem):
        pltpu.make_async_copy(ref, ref, sem).wait()

    def first(n, carry):
        send_raw(n)
        return carry

    lax.fori_loop(0, ahead, first, 0)
    for copy in locals_:
        copy.wait()
    wait_bytes(raw_ids.at[pl.ds(0, plane - 1)], ids_got)

    def finish(i):
        for d in range(lines - 1):
            wait_bytes(got_parts.at[i, d], parts_got.at[i, d])
            wait_bytes(got_scales.at[i, d], scales_got.at[i, d])

        def table(kk, carry):
            at = i * batch + kk
            total = own[at]
            for d in range(lines - 1):
                far = got_parts[i, d, kk].astype(jnp.int32).astype(jnp.float32)
                total += far * got_scales[i, d, kk, 0:1, :]
            square = jnp.sum(total * total, axis=0, keepdims=True) * (1.0 / width)
            sums = held_accum[pl.ds(at, 1), :] + square
            made_accum[pl.ds(at, 1), :] = sums
            step_size = LEARN_RATE / (jnp.sqrt(sums) + EPSILON)
            change = (total * step_size).T
            made_weights[at] = (held_weights[at].astype(jnp.float32) - change).astype(jnp.bfloat16)
            return carry

        lax.fori_loop(0, batch, table, 0)
        mine = pl.ds(i * batch, batch)
        for o in range(1, groups):
            pltpu.make_async_remote_copy(
                src_ref=made_weights.at[mine], dst_ref=new_weights.at[g, mine],
                send_sem=weights_sent, recv_sem=weights_got.at[o - 1],
                device_id=((g + o) % groups, s), device_id_type=MESH,
            ).start()
        pltpu.make_async_copy(made_weights.at[mine], new_weights.at[g, mine], local.at[4]).start()

    def step(n, carry):
        i, d = n // lines, n % lines
        a = place_of(n)

        @pl.when(n + ahead < steps)
        def _():
            wait_bytes(raw.at[a, pl.ds(0, plane - 1)], raw_sent.at[n % ahead])
            send_raw(n + ahead)

        wait_bytes(raw.at[a, pl.ds(0, plane - 1)], raw_got.at[a])

        def table(kk, carry):
            sum_rows(
                lambda b: raw_ids[b, a, kk],
                lambda b, many: raw[a, b : b + many, kk].reshape(many * samples, width),
                plane, counts, acc, offset,
            )

            @pl.when(d < lines - 1)
            def _():
                value = acc[...]
                top = jnp.maximum(jnp.max(jnp.abs(value), axis=0, keepdims=True), SMALLEST)
                coded = jnp.round(value * (LEVELS / top))
                parts[i, d, kk] = coded.astype(jnp.int32).astype(jnp.int16)
                scales[i, d, kk] = jnp.broadcast_to(top * (1.0 / LEVELS), (8, row_count))

            @pl.when(d == lines - 1)
            def _():
                own[i * batch + kk] = acc[...]

            return carry

        lax.fori_loop(0, batch, table, 0)

        @pl.when(d < lines - 1)
        def _():
            device = in_line(d)[1]
            pltpu.make_async_remote_copy(
                src_ref=parts.at[i, d], dst_ref=got_parts.at[i, d],
                send_sem=parts_sent, recv_sem=parts_got.at[i, d],
                device_id=device, device_id_type=MESH,
            ).start()
            pltpu.make_async_remote_copy(
                src_ref=scales.at[i, d], dst_ref=got_scales.at[i, d],
                send_sem=scales_sent, recv_sem=scales_got.at[i, d],
                device_id=device, device_id_type=MESH,
            ).start()

        @pl.when((d == lines - 1) & (i > 0))
        def _():
            finish(i - 1)

        return carry

    lax.fori_loop(0, steps, step, 0)
    finish(rounds - 1)

    for o in range(1, groups):
        pltpu.make_async_remote_copy(
            src_ref=made_accum, dst_ref=new_accum.at[g],
            send_sem=accum_sent, recv_sem=accum_got.at[o - 1],
            device_id=((g + o) % groups, s), device_id_type=MESH,
        ).start()
    last = pltpu.make_async_copy(made_accum, new_accum.at[g], local.at[5])
    last.start()

    def drain(n, carry):
        wait_bytes(raw.at[0, pl.ds(0, plane - 1)], raw_sent.at[n])
        return carry

    lax.fori_loop(0, ahead, drain, 0)
    wait_bytes(raw_ids.at[pl.ds(0, plane - 1)], ids_sent)
    wait_bytes(parts, parts_sent)
    wait_bytes(scales, scales_sent)
    wait_bytes(new_weights.at[g], local.at[4])
    last.wait()
    wait_bytes(new_weights.at[pl.ds(0, groups - 1)], weights_sent)
    wait_bytes(new_accum.at[pl.ds(0, groups - 1)], accum_sent)
    for o in range(1, groups):
        wait_bytes(new_weights.at[g], weights_got.at[o - 1])
        wait_bytes(new_accum.at[g], accum_got.at[o - 1])


def exchange(sends, ids, weights, accum, cores, lines, offset):
    steps, plane, batch, samples, width = sends.shape
    groups, quarter, row_count, _ = weights.shape
    bag = ids.shape[-2]
    rounds = steps // lines
    ahead = min(STEPS_AHEAD, steps)
    far = max(lines - 1, 1)
    unroll = 4 if plane % 4 == 0 else 1
    dma = pltpu.SemaphoreType.DMA
    anywhere = pl.BlockSpec(memory_space=pl.ANY)
    return pl.pallas_call(
        functools.partial(exchange_kernel, cores, lines, offset),
        in_specs=[anywhere] * 4,
        out_specs=[anywhere] * 2,
        out_shape=[
            jax.ShapeDtypeStruct(weights.shape, weights.dtype),
            jax.ShapeDtypeStruct(accum.shape, accum.dtype),
        ],
        scratch_shapes=[
            pltpu.VMEM((steps, plane, batch, samples, width), sends.dtype),
            pltpu.VMEM((plane, steps, batch, bag, samples), ids.dtype),
            pltpu.VMEM((row_count, unroll * samples), jnp.bfloat16),
            pltpu.VMEM((width, row_count), jnp.float32),
            pltpu.VMEM((rounds, far, batch, width, row_count), jnp.int16),
            pltpu.VMEM((rounds, far, batch, 8, row_count), jnp.float32),
            pltpu.VMEM((rounds, far, batch, width, row_count), jnp.int16),
            pltpu.VMEM((rounds, far, batch, 8, row_count), jnp.float32),
            pltpu.VMEM((quarter, width, row_count), jnp.float32),
            pltpu.VMEM((quarter, row_count, width), weights.dtype),
            pltpu.VMEM((quarter, row_count), jnp.float32),
            pltpu.VMEM((quarter, row_count, width), weights.dtype),
            pltpu.VMEM((quarter, row_count), jnp.float32),
            dma((ahead,)), dma((steps,)), dma, dma, dma((6,)),
            dma, dma((rounds, far)), dma, dma((rounds, far)),
            dma, dma((groups - 1,)), dma, dma((groups - 1,)),
        ],
        compiler_params=pltpu.CompilerParams(
            collective_id=0, has_side_effects=True, vmem_limit_bytes=60 * 2**20
        ),
    )(sends, ids, weights, accum)


def body(grad_pooled, bag_rows, bag_lengths, table_order, weights, accum):
    held, row_count, width = weights.shape
    samples, tables, _ = grad_pooled.shape
    bag = bag_rows.shape[2]
    groups = lax.axis_size("group")
    shards = lax.axis_size("shard")
    cores = 2 if shards % 2 == 0 else 1
    lines = shards // cores
    plane = groups * cores
    quarter = held // groups
    batch = 2 if quarter % 2 == 0 else 1
    rounds = quarter // batch
    steps = lines * rounds
    offset = row_count // 2

    by_slot = table_order.reshape(lines, cores, groups, rounds, batch)
    by_step = by_slot.transpose(0, 3, 2, 1, 4).reshape(-1)
    by_device = by_slot.transpose(2, 1, 0, 3, 4).reshape(-1)

    live = jnp.arange(bag, dtype=jnp.int32)[None, :, None] < bag_lengths[:, None, :]
    ids = jnp.where(live, jnp.transpose(bag_rows, (0, 2, 1)), row_count) - offset
    ids = jnp.transpose(ids.astype(jnp.float32), (2, 1, 0))
    ids = jnp.take(ids, by_device, axis=0, mode="clip", unique_indices=True).astype(jnp.bfloat16)
    ids = ids.reshape(plane, steps, batch, bag, samples)

    sends = arrange(grad_pooled, by_step).reshape(steps, plane, batch, samples, width)
    new_weights, new_accum = exchange(
        sends, ids,
        weights.reshape(groups, quarter, row_count, width),
        accum.reshape(groups, quarter, row_count),
        cores, lines, offset,
    )
    return new_weights.reshape(weights.shape), new_accum.reshape(accum.shape)


def solution(mesh):
    in_specs = (
        P(AXES, None, None),
        P(AXES, None, None),
        P(AXES, None),
        P(),
        P("shard", None, None),
        P("shard", None),
    )
    out_specs = (P("shard", None, None), P("shard", None))
    return jax.shard_map(body, mesh=mesh, in_specs=in_specs, out_specs=out_specs, check_vma=False)
```

```python
import functools

import jax
import jax.numpy as jnp
import numpy as np
from jax import lax
from jax.experimental import pallas as pl
from jax.experimental.pallas import tpu as pltpu
from jax.sharding import PartitionSpec as P

LEARN_RATE = 0.5
EPSILON = 1e-06
AXES = ("group", "shard")
TILE = 16
BLOCK = 32
STEPS_AHEAD = 8
PASS_AFTER = 4
FINISH_AFTER = 0
SPAN = 4
LEVELS = 32760.0
SMALLEST = 1e-30
MESH = pl.DeviceIdType.MESH


def arrange_kernel(place_ref, grad_ref, out_ref):
    tables = grad_ref.shape[1]

    def flip(step, carry):
        start = pl.multiple_of(step * TILE, TILE)
        block = jnp.swapaxes(grad_ref[:, pl.ds(start, TILE), :], 0, 1)
        for k in range(TILE):
            out_ref[place_ref[start + k]] = block[k]
        return carry

    lax.fori_loop(0, tables // TILE, flip, 0)


def arrange(grad_pooled, places):
    samples, tables, width = grad_pooled.shape
    block = BLOCK if samples % BLOCK == 0 else TILE
    return pl.pallas_call(
        arrange_kernel,
        grid_spec=pltpu.PrefetchScalarGridSpec(
            num_scalar_prefetch=1,
            grid=(samples // block,),
            in_specs=[pl.BlockSpec((block, tables, width), lambda b, places: (b, 0, 0))],
            out_specs=pl.BlockSpec((tables, block, width), lambda b, places: (0, b, 0)),
        ),
        out_shape=jax.ShapeDtypeStruct((tables, samples, width), grad_pooled.dtype),
        cost_estimate=pl.CostEstimate(
            flops=0, bytes_accessed=4 * grad_pooled.size, transcendentals=0
        ),
    )(places, grad_pooled)


def sum_rows(load_ids, load_values, sources, counts, acc, offset):
    row_count, wide = counts.shape
    bag, samples = load_ids(0).shape
    unroll = wide // samples
    place = lax.broadcasted_iota(jnp.int32, (TILE, samples), 0).astype(jnp.float32)
    places = [(place + float(r * TILE - offset)).astype(jnp.bfloat16) for r in range(row_count // TILE)]
    one = jnp.ones((TILE, samples), jnp.bfloat16)
    zero = jnp.zeros((TILE, samples), jnp.bfloat16)
    for turn in range(sources // unroll):
        for u in range(unroll):
            picks = load_ids(turn * unroll + u).astype(jnp.float32)
            spread = [
                jnp.broadcast_to(picks[j : j + 1], (TILE, samples)).astype(jnp.bfloat16)
                for j in range(bag)
            ]
            for r, here in enumerate(places):
                terms = [jnp.where(s == here, one, zero) for s in spread]
                while len(terms) > 1:
                    terms = [a + b for a, b in zip(terms[::2], terms[1::2])] + (
                        [terms[-1]] if len(terms) % 2 else []
                    )
                counts[r * TILE : (r + 1) * TILE, u * samples : (u + 1) * samples] = terms[0]
        values = load_values(turn * unroll, unroll)
        part = lax.dot_general(
            values, counts[...], (((0,), (1,)), ((), ())), preferred_element_type=jnp.float32
        )
        if turn == 0:
            acc[...] = part
        else:
            acc[...] += part


class Split:
    def __init__(self, groups, shards):
        self.cores = 2 if shards % 2 == 0 else 1
        self.low = 2 if groups % 2 == 0 else 1
        self.near = 2 if (shards // self.cores) % 2 == 0 else 1
        self.groups = groups
        self.lines = shards // self.cores
        self.plane = groups * self.cores
        self.square = groups == 4 and self.low == 2
        self.mixed = self.square and self.near == 2
        self.span = SPAN if self.mixed else 1

    def turn(self, n, rounds):
        full = rounds // self.span * self.span
        block = self.span * self.lines
        if full == 0:
            return n % rounds, n // rounds
        short = n // (full * self.lines)
        many = self.span + (rounds - full - self.span) * short
        at = n - n // block * block
        return n // block * self.span + at % many, at // many

    def masks(self, i):
        if not self.mixed:
            return 1, 0, 0
        m = (i % 2) * (1 + i % 4 // 2)
        return (m - 1) * (m - 2) // 2, m * (2 - m), m * (m - 1) // 2

    def here(self, i, g, s):
        flat, swap_high, swap_low = self.masks(i)
        z, c = s // self.cores, s % self.cores
        high, low = g // self.low, g % self.low
        far, near = z // self.near, z % self.near
        first = high * (1 - swap_high) + near * swap_high
        second = low * (1 - swap_low) + near * swap_low
        rest = near * flat + high * swap_high + low * swap_low
        return (first * self.low + second) * self.cores + c, far * self.near + rest

    def device(self, i, p, line):
        flat, swap_high, swap_low = self.masks(i)
        c, pair = p % self.cores, p // self.cores
        first, second = pair // self.low, pair % self.low
        far, rest = line // self.near, line % self.near
        high = first * (1 - swap_high) + rest * swap_high
        low = second * (1 - swap_low) + rest * swap_low
        near = rest * flat + first * swap_high + second * swap_low
        return high * self.low + low, (far * self.near + near) * self.cores + c


def exchange_kernel(
    split, offset,
    sends, ids, weights, accum, new_weights, new_accum,
    raw, raw_ids, counts, acc, parts, scales, got_parts, got_scales, own,
    held_weights, held_accum, made_weights, made_accum,
    raw_sent, raw_got, raw_kept, ids_sent, ids_got, ids_kept, local,
    parts_sent, parts_got, scales_sent, scales_got,
    weights_sent, weights_got, passed_got, accum_sent, accum_got,
):
    steps, plane, batch = sends.shape[:3]
    groups, lines = split.groups, split.lines
    rounds = steps // lines
    ahead = raw_sent.shape[0]
    block = split.span * lines
    width, row_count = acc.shape
    g = lax.axis_index("group")
    s = lax.axis_index("shard")
    z = s // split.cores

    def remote(src, dst, sent, got, device):
        return pltpu.make_async_remote_copy(
            src_ref=src, dst_ref=dst, send_sem=sent, recv_sem=got,
            device_id=device, device_id_type=MESH,
        )

    def wait_bytes(ref, sem):
        pltpu.make_async_copy(ref, ref, sem).wait()

    barrier = pltpu.get_barrier_semaphore()
    greeted = 0
    for kind in (0, 1, 3) if split.mixed else (0,):
        p, line = split.here(kind, g, s)
        for o in range(1, plane):
            pl.semaphore_signal(
                barrier, inc=1, device_id=split.device(kind, (p + o) % plane, line),
                device_id_type=MESH,
            )
        for d in range(lines - 1):
            pl.semaphore_signal(
                barrier, inc=1, device_id=split.device(kind, p, (line + 1 + d) % lines),
                device_id_type=MESH,
            )
        greeted += plane - 1 + lines - 1

    held = [
        pltpu.make_async_copy(weights.at[g], held_weights, local.at[0]),
        pltpu.make_async_copy(accum.at[g], held_accum, local.at[1]),
    ]
    for copy in held:
        copy.start()
    pl.semaphore_wait(barrier, greeted)

    def place_of(n):
        i, d = split.turn(n, rounds)
        p, line = split.here(i, g, s)
        return i, d, p, line, (line + 1 + d) % lines

    def send_raw(n):
        i, d, p, line, to = place_of(n)

        @pl.when(d == 0)
        def _():
            for o in range(1, plane):
                q = (p + o) % plane
                remote(
                    ids.at[i, :, q], raw_ids.at[i, :, p], ids_sent, ids_got.at[i],
                    split.device(i, q, line),
                ).start()
            pltpu.make_async_copy(ids.at[i, :, p], raw_ids.at[i, :, p], ids_kept.at[i]).start()

        a = i * lines + to
        for o in range(1, plane):
            q = (p + o) % plane
            remote(
                sends.at[a, q], raw.at[a, p], raw_sent.at[n % ahead], raw_got.at[a],
                split.device(i, q, line),
            ).start()
        pltpu.make_async_copy(sends.at[a, p], raw.at[a, p], raw_kept.at[n % ahead]).start()

    def first(n, carry):
        send_raw(n)
        return carry

    lax.fori_loop(0, ahead, first, 0)
    for copy in held:
        copy.wait()
    others = pl.ds(0, plane - 1)
    beside = (g // split.low) * split.low + (g % split.low + 1) % split.low
    across = (g + split.low) % groups
    half = row_count // 2

    def finish(i):
        for d in range(lines - 1):
            wait_bytes(got_parts.at[i, d], parts_got.at[i, d])
            wait_bytes(got_scales.at[i, d], scales_got.at[i, d])

        def table(kk, carry):
            at = i * batch + kk
            total = own[at]
            for d in range(lines - 1):
                far = got_parts[i, d, kk].astype(jnp.int32).astype(jnp.float32)
                total += far * got_scales[i, d, pl.ds(kk, 1), :]
            square = jnp.sum(total * total, axis=0, keepdims=True) * (1.0 / width)
            sums = held_accum[pl.ds(at, 1), :] + square
            made_accum[pl.ds(at, 1), :] = sums
            step_size = LEARN_RATE / (jnp.sqrt(sums) + EPSILON)
            change = (total * step_size).T
            made_weights[at] = (held_weights[at].astype(jnp.float32) - change).astype(jnp.bfloat16)
            return carry

        lax.fori_loop(0, batch, table, 0)
        mine = pl.ds(i * batch, batch)
        if split.square:
            targets = [beside, across]
        else:
            targets = [(g + o) % groups for o in range(1, groups)]
        for at, to in enumerate(targets):
            remote(
                made_weights.at[mine], new_weights.at[g, mine],
                weights_sent, weights_got.at[i, at], (to, s),
            ).start()
        pltpu.make_async_copy(made_weights.at[mine], new_weights.at[g, mine], local.at[2]).start()

    def pass_on(i):
        if not split.square:
            return
        mine = pl.ds(i * batch, batch)
        for at, (source, to) in enumerate(((beside, across), (across, beside))):
            wait_bytes(new_weights.at[source, mine], weights_got.at[i, at])
            rows = new_weights.at[source, mine, pl.ds(at * half, half)]
            remote(rows, rows, weights_sent, passed_got.at[at], (to, s)).start()

    def step(n, carry):
        i, d, p, line, to = place_of(n)
        a = i * lines + to

        wait_bytes(raw.at[a, p], raw_kept.at[n % ahead])

        @pl.when(n + ahead < steps)
        def _():
            wait_bytes(raw.at[a, others], raw_sent.at[n % ahead])
            send_raw(n + ahead)

        @pl.when(d == 0)
        def _():
            wait_bytes(raw_ids.at[i, :, p], ids_kept.at[i])
            wait_bytes(raw_ids.at[i, :, others], ids_got.at[i])

        wait_bytes(raw.at[a, others], raw_got.at[a])

        def table(kk, carry):
            sum_rows(
                lambda b: raw_ids[i, to, b, kk],
                lambda b, many: raw[a, b : b + many, kk].reshape(many * samples, width),
                plane, counts, acc, offset,
            )

            @pl.when(d < lines - 1)
            def _():
                value = acc[...]
                top = jnp.maximum(jnp.max(jnp.abs(value), axis=0, keepdims=True), SMALLEST)
                coded = jnp.round(value * (LEVELS / top))
                parts[i, d, kk] = coded.astype(jnp.int32).astype(jnp.int16)
                scales[i, d, pl.ds(kk, 1), :] = top * (1.0 / LEVELS)

            @pl.when(d == lines - 1)
            def _():
                own[i * batch + kk] = acc[...]

            return carry

        samples = raw.shape[3]
        lax.fori_loop(0, batch, table, 0)

        @pl.when(d < lines - 1)
        def _():
            device = split.device(i, p, to)
            remote(
                parts.at[i, d], got_parts.at[i, d], parts_sent, parts_got.at[i, d], device
            ).start()
            remote(
                scales.at[i, d], got_scales.at[i, d], scales_sent, scales_got.at[i, d], device
            ).start()

        back = n - block - FINISH_AFTER
        done = back // block * split.span

        @pl.when((back >= 0) & (back % block < split.span))
        def _():
            finish(done + back % block)

        later = back - PASS_AFTER

        @pl.when((later >= 0) & (later % block < split.span))
        def _():
            pass_on(later // block * split.span + later % block)

        return carry

    lax.fori_loop(0, steps, step, 0)
    due = [i // split.span * block + block + i % split.span + FINISH_AFTER for i in range(rounds)]
    for i in range(rounds):
        if due[i] >= steps:
            finish(i)
        elif due[i] + PASS_AFTER >= steps:
            pass_on(i)

    for o in range(1, groups):
        remote(
            made_accum, new_accum.at[g], accum_sent, accum_got.at[o - 1], ((g + o) % groups, s)
        ).start()
    last = pltpu.make_async_copy(made_accum, new_accum.at[g], local.at[3])
    last.start()
    for i in range(rounds):
        if due[i] >= steps:
            pass_on(i)

    def drain(n, carry):
        wait_bytes(raw.at[0, others], raw_sent.at[n])
        return carry

    lax.fori_loop(0, ahead, drain, 0)
    wait_bytes(raw_ids.at[:, :, others], ids_sent)
    wait_bytes(parts, parts_sent)
    wait_bytes(scales, scales_sent)
    wait_bytes(new_weights.at[g], local.at[2])
    last.wait()
    wait_bytes(new_weights.at[pl.ds(0, groups - 1)], weights_sent)
    wait_bytes(new_accum.at[pl.ds(0, groups - 1)], accum_sent)
    for o in range(1, groups):
        wait_bytes(new_accum.at[g], accum_got.at[o - 1])
    if split.square:
        for at in range(2):
            wait_bytes(new_weights.at[g, :, pl.ds(0, half)], passed_got.at[at])
    else:
        for i in range(rounds):
            for o in range(1, groups):
                wait_bytes(new_weights.at[g, pl.ds(i * batch, batch)], weights_got.at[i, o - 1])


def exchange(sends, ids, weights, accum, split, offset):
    steps, plane, batch, samples, width = sends.shape
    groups, quarter, row_count, _ = weights.shape
    bag = ids.shape[-2]
    lines = split.lines
    rounds = steps // lines
    ahead = min(STEPS_AHEAD, steps)
    far = max(lines - 1, 1)
    unroll = 4 if plane % 4 == 0 else 1
    dma = pltpu.SemaphoreType.DMA
    anywhere = pl.BlockSpec(memory_space=pl.ANY)
    return pl.pallas_call(
        functools.partial(exchange_kernel, split, offset),
        in_specs=[anywhere] * 4,
        out_specs=[anywhere] * 2,
        out_shape=[
            jax.ShapeDtypeStruct(weights.shape, weights.dtype),
            jax.ShapeDtypeStruct(accum.shape, accum.dtype),
        ],
        scratch_shapes=[
            pltpu.VMEM((steps, plane, batch, samples, width), sends.dtype),
            pltpu.VMEM((rounds, lines, plane, batch, bag, samples), ids.dtype),
            pltpu.VMEM((row_count, unroll * samples), jnp.bfloat16),
            pltpu.VMEM((width, row_count), jnp.float32),
            pltpu.VMEM((rounds, far, batch, width, row_count), jnp.int16),
            pltpu.VMEM((rounds, far, 8, row_count), jnp.float32),
            pltpu.VMEM((rounds, far, batch, width, row_count), jnp.int16),
            pltpu.VMEM((rounds, far, 8, row_count), jnp.float32),
            pltpu.VMEM((quarter, width, row_count), jnp.float32),
            pltpu.VMEM((quarter, row_count, width), weights.dtype),
            pltpu.VMEM((quarter, row_count), jnp.float32),
            pltpu.VMEM((quarter, row_count, width), weights.dtype),
            pltpu.VMEM((quarter, row_count), jnp.float32),
            dma((ahead,)), dma((steps,)), dma((ahead,)), dma, dma((rounds,)), dma((rounds,)),
            dma((4,)),
            dma, dma((rounds, far)), dma, dma((rounds, far)),
            dma, dma((rounds, groups - 1)), dma((2,)), dma, dma((groups - 1,)),
        ],
        compiler_params=pltpu.CompilerParams(
            collective_id=0, has_side_effects=True, vmem_limit_bytes=60 * 2**20
        ),
    )(sends, ids, weights, accum)


def body(grad_pooled, bag_rows, bag_lengths, table_order, weights, accum):
    held, row_count, width = weights.shape
    samples, tables, _ = grad_pooled.shape
    bag = bag_rows.shape[2]
    split = Split(lax.axis_size("group"), lax.axis_size("shard"))
    groups, lines, plane = split.groups, split.lines, split.plane
    quarter = held // groups
    batch = 2 if quarter % 32 == 0 else 1
    rounds = quarter // batch
    steps = lines * rounds
    offset = row_count // 2

    i, line, p, k = np.meshgrid(*map(np.arange, (rounds, lines, plane, batch)), indexing="ij")
    group, shard = split.device(i, p, line)
    slots = (shard * held + group * quarter + i * batch + k).reshape(-1)
    numbers = np.arange(tables)
    from_slot = jnp.asarray(slots[:, None] == numbers[None, :])
    order = jnp.sum(jnp.where(from_slot, table_order[None, :], 0), axis=1)
    at_slot = jnp.asarray(np.argsort(slots), jnp.int32)
    table_at = table_order[None, :] == jnp.arange(tables, dtype=jnp.int32)[:, None]
    places = jnp.sum(jnp.where(table_at, at_slot[None, :], 0), axis=1)

    live = jnp.arange(bag, dtype=jnp.int32)[None, :, None] < bag_lengths[:, None, :]
    ids = jnp.where(live, jnp.transpose(bag_rows, (0, 2, 1)), row_count) - offset
    ids = jnp.transpose(ids.astype(jnp.float32), (2, 1, 0))
    ids = jnp.take(ids, order, axis=0, mode="clip", unique_indices=True).astype(jnp.bfloat16)
    ids = ids.reshape(rounds, lines, plane, batch, bag, samples)

    sends = arrange(grad_pooled, places).reshape(steps, plane, batch, samples, width)
    new_weights, new_accum = exchange(
        sends, ids,
        weights.reshape(groups, quarter, row_count, width),
        accum.reshape(groups, quarter, row_count),
        split, offset,
    )
    return new_weights.reshape(weights.shape), new_accum.reshape(accum.shape)


def solution(mesh):
    in_specs = (
        P(AXES, None, None),
        P(AXES, None, None),
        P(AXES, None),
        P(),
        P("shard", None, None),
        P("shard", None),
    )
    out_specs = (P("shard", None, None), P("shard", None))
    return jax.shard_map(body, mesh=mesh, in_specs=in_specs, out_specs=out_specs, check_vma=False)
```

```python
import functools

import jax
import jax.numpy as jnp
import numpy as np
from jax import lax
from jax.experimental import pallas as pl
from jax.experimental.pallas import tpu as pltpu
from jax.sharding import PartitionSpec as P

LEARN_RATE = 0.5
EPSILON = 1e-06
AXES = ("group", "shard")
TILE = 16
BLOCK = 32
STEPS_AHEAD = 8
PASS_AFTER = 4
NARROW = 2
NARROW_ROUNDS = 4
SPAN = 4
LEVELS = 32760.0
SMALLEST = 1e-30
MESH = pl.DeviceIdType.MESH


def arrange_kernel(place_ref, grad_ref, out_ref):
    tables = grad_ref.shape[1]

    def flip(step, carry):
        start = pl.multiple_of(step * TILE, TILE)
        block = jnp.swapaxes(grad_ref[:, pl.ds(start, TILE), :], 0, 1)
        for k in range(TILE):
            out_ref[place_ref[start + k]] = block[k]
        return carry

    lax.fori_loop(0, tables // TILE, flip, 0)


def arrange(grad_pooled, places):
    samples, tables, width = grad_pooled.shape
    block = BLOCK if samples % BLOCK == 0 else TILE
    return pl.pallas_call(
        arrange_kernel,
        grid_spec=pltpu.PrefetchScalarGridSpec(
            num_scalar_prefetch=1,
            grid=(samples // block,),
            in_specs=[pl.BlockSpec((block, tables, width), lambda b, places: (b, 0, 0))],
            out_specs=pl.BlockSpec((tables, block, width), lambda b, places: (0, b, 0)),
        ),
        out_shape=jax.ShapeDtypeStruct((tables, samples, width), grad_pooled.dtype),
        cost_estimate=pl.CostEstimate(
            flops=0, bytes_accessed=4 * grad_pooled.size, transcendentals=0
        ),
    )(places, grad_pooled)


def sum_rows(load_ids, load_values, sources, counts, acc, offset):
    row_count, wide = counts.shape
    bag, samples = load_ids(0).shape
    unroll = wide // samples
    place = lax.broadcasted_iota(jnp.int32, (TILE, samples), 0).astype(jnp.float32)
    places = [(place + float(r * TILE - offset)).astype(jnp.bfloat16) for r in range(row_count // TILE)]
    one = jnp.ones((TILE, samples), jnp.bfloat16)
    zero = jnp.zeros((TILE, samples), jnp.bfloat16)
    for turn in range(sources // unroll):
        for u in range(unroll):
            picks = load_ids(turn * unroll + u).astype(jnp.float32)
            spread = [
                jnp.broadcast_to(picks[j : j + 1], (TILE, samples)).astype(jnp.bfloat16)
                for j in range(bag)
            ]
            for r, here in enumerate(places):
                terms = [jnp.where(s == here, one, zero) for s in spread]
                while len(terms) > 1:
                    terms = [a + b for a, b in zip(terms[::2], terms[1::2])] + (
                        [terms[-1]] if len(terms) % 2 else []
                    )
                counts[r * TILE : (r + 1) * TILE, u * samples : (u + 1) * samples] = terms[0]
        values = load_values(turn * unroll, unroll)
        part = lax.dot_general(
            values, counts[...], (((0,), (1,)), ((), ())), preferred_element_type=jnp.float32
        )
        if turn == 0:
            acc[...] = part
        else:
            acc[...] += part


class Split:
    def __init__(self, groups, shards):
        self.cores = 2 if shards % 2 == 0 else 1
        self.low = 2 if groups % 2 == 0 else 1
        self.near = 2 if (shards // self.cores) % 2 == 0 else 1
        self.groups = groups
        self.lines = shards // self.cores
        self.plane = groups * self.cores
        self.square = groups == 4 and self.low == 2
        self.mixed = self.square and self.near == 2
        self.span = SPAN if self.mixed else 1

    def spans(self, rounds):
        wide = max(rounds - NARROW_ROUNDS, 0) // self.span * self.span
        narrow = NARROW if self.mixed and (rounds - wide) % NARROW == 0 else 1
        return wide, narrow

    def turn(self, n, rounds):
        wide, narrow = self.spans(rounds)
        steps = rounds * self.lines
        if wide == 0:
            late, many, at = 1, narrow, n
        else:
            late = (n + steps - wide * self.lines) // steps
            many = self.span + (narrow - self.span) * late
            at = n - wide * self.lines * late
        block = many * self.lines
        return wide * late + at // block * many + at % many, at % block // many

    def due(self, i, rounds):
        wide, narrow = self.spans(rounds)
        base, many = (0, self.span) if i < wide else (wide, narrow)
        return (base + (i - base) // many * many + many) * self.lines + (i - base) % many

    def masks(self, i):
        if not self.mixed:
            return 1, 0, 0
        m = (i % 2) * (1 + i % 4 // 2)
        return (m - 1) * (m - 2) // 2, m * (2 - m), m * (m - 1) // 2

    def here(self, i, g, s):
        flat, swap_high, swap_low = self.masks(i)
        z, c = s // self.cores, s % self.cores
        high, low = g // self.low, g % self.low
        far, near = z // self.near, z % self.near
        first = high * (1 - swap_high) + near * swap_high
        second = low * (1 - swap_low) + near * swap_low
        rest = near * flat + high * swap_high + low * swap_low
        return (first * self.low + second) * self.cores + c, far * self.near + rest

    def device(self, i, p, line):
        flat, swap_high, swap_low = self.masks(i)
        c, pair = p % self.cores, p // self.cores
        first, second = pair // self.low, pair % self.low
        far, rest = line // self.near, line % self.near
        high = first * (1 - swap_high) + rest * swap_high
        low = second * (1 - swap_low) + rest * swap_low
        near = rest * flat + first * swap_high + second * swap_low
        return high * self.low + low, (far * self.near + near) * self.cores + c


def exchange_kernel(
    split, offset,
    order, sends, bag_rows, bag_lengths, weights, accum, new_weights, new_accum,
    raw, raw_ids, rows, lengths, by_table, ids, counts, acc, parts, scales, got_parts, got_scales, own,
    held_weights, held_accum, made_accum,
    raw_sent, raw_got, raw_kept, ids_sent, ids_got, local,
    parts_sent, parts_got, scales_sent, scales_got,
    weights_sent, weights_got, passed_got, accum_sent, accum_got,
):
    steps, plane, batch = sends.shape[:3]
    groups, lines = split.groups, split.lines
    rounds = steps // lines
    ahead = raw_sent.shape[0]
    wide, narrow = split.spans(rounds)
    width, row_count = acc.shape
    g = lax.axis_index("group")
    s = lax.axis_index("shard")
    z = s // split.cores

    def remote(src, dst, sent, got, device):
        return pltpu.make_async_remote_copy(
            src_ref=src, dst_ref=dst, send_sem=sent, recv_sem=got,
            device_id=device, device_id_type=MESH,
        )

    def wait_bytes(ref, sem):
        pltpu.make_async_copy(ref, ref, sem).wait()

    barrier = pltpu.get_barrier_semaphore()
    greeted = 0
    for kind in (0, 1, 3) if split.mixed else (0,):
        p, line = split.here(kind, g, s)
        for o in range(1, plane):
            pl.semaphore_signal(
                barrier, inc=1, device_id=split.device(kind, (p + o) % plane, line),
                device_id_type=MESH,
            )
        for d in range(lines - 1):
            pl.semaphore_signal(
                barrier, inc=1, device_id=split.device(kind, p, (line + 1 + d) % lines),
                device_id_type=MESH,
            )
        greeted += plane - 1 + lines - 1

    held = [
        pltpu.make_async_copy(weights.at[g], held_weights, local.at[0]),
        pltpu.make_async_copy(accum.at[g], held_accum, local.at[1]),
        pltpu.make_async_copy(bag_rows, rows, local.at[2]),
        pltpu.make_async_copy(bag_lengths, lengths, local.at[4]),
    ]
    for copy in held:
        copy.start()
    pl.semaphore_wait(barrier, greeted)

    def place_of(n):
        i, d = split.turn(n, rounds)
        p, line = split.here(i, g, s)
        return i, d, p, line, (line + 1 + d) % lines

    def send_raw(n):
        i, d, p, line, to = place_of(n)
        a = i * lines + to
        for o in range(1, plane):
            q = (p + o) % plane
            remote(
                sends.at[a, q], raw.at[a, p], raw_sent.at[n % ahead], raw_got.at[a],
                split.device(i, q, line),
            ).start()
        pltpu.make_async_copy(sends.at[a, p], raw.at[a, p], raw_kept.at[n % ahead]).start()

    def first(n, carry):
        send_raw(n)
        return carry

    lax.fori_loop(0, ahead, first, 0)
    for copy in held:
        copy.wait()

    bag = rows.shape[1]
    for j in range(bag):
        live = jnp.where(lengths[...] > j, rows[:, j, :], row_count) - offset
        by_table[:, j, :] = live.astype(jnp.float32).T

    def gather(step, carry):
        i, to = step // lines, step % lines
        for q in range(plane):
            for kk in range(batch):
                at = (step * plane + q) * batch + kk
                ids[i, to, q, kk] = by_table[order[at]].astype(jnp.bfloat16)
        return carry

    lax.fori_loop(0, steps, gather, 0)

    def send_ids(i, carry):
        p, line = split.here(i, g, s)
        for o in range(1, plane):
            q = (p + o) % plane
            remote(
                ids.at[i, :, q], raw_ids.at[i, :, p], ids_sent, ids_got.at[i],
                split.device(i, q, line),
            ).start()
        return carry

    lax.fori_loop(0, rounds, send_ids, 0)
    others = pl.ds(0, plane - 1)
    beside = (g // split.low) * split.low + (g % split.low + 1) % split.low
    across = (g + split.low) % groups
    half = row_count // 2

    def finish(i):
        for d in range(lines - 1):
            wait_bytes(got_parts.at[i, d], parts_got.at[i, d])
            wait_bytes(got_scales.at[i, d], scales_got.at[i, d])

        def table(kk, carry):
            at = i * batch + kk
            total = own[at]
            for d in range(lines - 1):
                far = got_parts[i, d, kk].astype(jnp.int32).astype(jnp.float32)
                total += far * got_scales[i, d, pl.ds(kk, 1), :]
            square = jnp.sum(total * total, axis=0, keepdims=True) * (1.0 / width)
            sums = held_accum[pl.ds(at, 1), :] + square
            made_accum[pl.ds(at, 1), :] = sums
            step_size = LEARN_RATE / (jnp.sqrt(sums) + EPSILON)
            change = (total * step_size).T
            new_weights[g, at] = (held_weights[at].astype(jnp.float32) - change).astype(jnp.bfloat16)
            return carry

        lax.fori_loop(0, batch, table, 0)
        mine = pl.ds(i * batch, batch)
        if split.square:
            targets = [beside, across]
        else:
            targets = [(g + o) % groups for o in range(1, groups)]
        for at, to in enumerate(targets):
            remote(
                new_weights.at[g, mine], new_weights.at[g, mine],
                weights_sent, weights_got.at[i, at], (to, s),
            ).start()

    def pass_on(i):
        if not split.square:
            return
        mine = pl.ds(i * batch, batch)
        for at, (source, to) in enumerate(((beside, across), (across, beside))):
            wait_bytes(new_weights.at[source, mine], weights_got.at[i, at])
            rows = new_weights.at[source, mine, pl.ds(at * half, half)]
            remote(rows, rows, weights_sent, passed_got.at[at], (to, s)).start()

    def step(n, carry):
        i, d, p, line, to = place_of(n)
        a = i * lines + to

        wait_bytes(raw.at[a, p], raw_kept.at[n % ahead])

        @pl.when(n + ahead < steps)
        def _():
            wait_bytes(raw.at[a, others], raw_sent.at[n % ahead])
            send_raw(n + ahead)

        @pl.when(d == 0)
        def _():
            wait_bytes(raw_ids.at[i, :, others], ids_got.at[i])
            raw_ids[i, :, p] = ids[i, :, p]

        wait_bytes(raw.at[a, others], raw_got.at[a])

        def table(kk, carry):
            sum_rows(
                lambda b: raw_ids[i, to, b, kk],
                lambda b, many: raw[a, b : b + many, kk].reshape(many * samples, width),
                plane, counts, acc, offset,
            )

            @pl.when(d < lines - 1)
            def _():
                value = acc[...]
                top = jnp.maximum(jnp.max(jnp.abs(value), axis=0, keepdims=True), SMALLEST)
                coded = jnp.round(value * (LEVELS / top))
                parts[i, d, kk] = coded.astype(jnp.int32).astype(jnp.int16)
                scales[i, d, pl.ds(kk, 1), :] = top * (1.0 / LEVELS)

            @pl.when(d == lines - 1)
            def _():
                own[i * batch + kk] = acc[...]

            return carry

        samples = raw.shape[3]
        lax.fori_loop(0, batch, table, 0)

        @pl.when(d < lines - 1)
        def _():
            device = split.device(i, p, to)
            remote(
                parts.at[i, d], got_parts.at[i, d], parts_sent, parts_got.at[i, d], device
            ).start()
            remote(
                scales.at[i, d], got_scales.at[i, d], scales_sent, scales_got.at[i, d], device
            ).start()

        for base, top, many in ((0, wide, split.span), (wide, rounds, narrow)):
            block = many * lines
            back = n - base * lines - block
            ready = base + back // block * many + back % block

            @pl.when((back >= 0) & (back % block < many) & (ready < top))
            def _():
                finish(ready)

            later = back - PASS_AFTER
            passed = base + later // block * many + later % block

            @pl.when((later >= 0) & (later % block < many) & (passed < top))
            def _():
                pass_on(passed)

        return carry

    lax.fori_loop(0, steps, step, 0)
    due = [split.due(i, rounds) for i in range(rounds)]
    for i in range(rounds):
        if due[i] >= steps:
            finish(i)
        elif due[i] + PASS_AFTER >= steps:
            pass_on(i)

    for o in range(1, groups):
        remote(
            made_accum, new_accum.at[g], accum_sent, accum_got.at[o - 1], ((g + o) % groups, s)
        ).start()
    last = pltpu.make_async_copy(made_accum, new_accum.at[g], local.at[3])
    last.start()
    for i in range(rounds):
        if due[i] >= steps:
            pass_on(i)

    def drain(n, carry):
        wait_bytes(raw.at[0, others], raw_sent.at[n])
        return carry

    lax.fori_loop(0, ahead, drain, 0)
    wait_bytes(raw_ids.at[:, :, others], ids_sent)
    wait_bytes(parts, parts_sent)
    wait_bytes(scales, scales_sent)
    last.wait()
    wait_bytes(new_weights.at[pl.ds(0, groups - 1)], weights_sent)
    wait_bytes(new_accum.at[pl.ds(0, groups - 1)], accum_sent)
    for o in range(1, groups):
        wait_bytes(new_accum.at[g], accum_got.at[o - 1])
    if split.square:
        for at in range(2):
            wait_bytes(new_weights.at[g, :, pl.ds(0, half)], passed_got.at[at])
    else:
        for i in range(rounds):
            for o in range(1, groups):
                wait_bytes(new_weights.at[g, pl.ds(i * batch, batch)], weights_got.at[i, o - 1])


def exchange(order, sends, bag_rows, bag_lengths, weights, accum, split, offset):
    steps, plane, batch, samples, width = sends.shape
    groups, quarter, row_count, _ = weights.shape
    bag = bag_rows.shape[1]
    lines = split.lines
    rounds = steps // lines
    ahead = min(STEPS_AHEAD, steps)
    far = max(lines - 1, 1)
    unroll = 4 if plane % 4 == 0 else 1
    dma = pltpu.SemaphoreType.DMA
    anywhere = pl.BlockSpec(memory_space=pl.ANY)
    return pl.pallas_call(
        functools.partial(exchange_kernel, split, offset),
        in_specs=[pl.BlockSpec(memory_space=pltpu.SMEM)] + [anywhere] * 5,
        out_specs=[pl.BlockSpec(memory_space=pltpu.VMEM), anywhere],
        out_shape=[
            pltpu.VMEM(weights.shape, weights.dtype),
            jax.ShapeDtypeStruct(accum.shape, accum.dtype),
        ],
        scratch_shapes=[
            pltpu.VMEM((steps, plane, batch, samples, width), sends.dtype),
            pltpu.VMEM((rounds, lines, plane, batch, bag, samples), jnp.bfloat16),
            pltpu.VMEM(bag_rows.shape, bag_rows.dtype),
            pltpu.VMEM(bag_lengths.shape, bag_lengths.dtype),
            pltpu.VMEM((bag_rows.shape[2], bag, samples), jnp.float32),
            pltpu.VMEM((rounds, lines, plane, batch, bag, samples), jnp.bfloat16),
            pltpu.VMEM((row_count, unroll * samples), jnp.bfloat16),
            pltpu.VMEM((width, row_count), jnp.float32),
            pltpu.VMEM((rounds, far, batch, width, row_count), jnp.int16),
            pltpu.VMEM((rounds, far, 8, row_count), jnp.float32),
            pltpu.VMEM((rounds, far, batch, width, row_count), jnp.int16),
            pltpu.VMEM((rounds, far, 8, row_count), jnp.float32),
            pltpu.VMEM((quarter, width, row_count), jnp.float32),
            pltpu.VMEM((quarter, row_count, width), weights.dtype),
            pltpu.VMEM((quarter, row_count), jnp.float32),
            pltpu.VMEM((quarter, row_count), jnp.float32),
            dma((ahead,)), dma((steps,)), dma((ahead,)), dma, dma((rounds,)),
            dma((5,)),
            dma, dma((rounds, far)), dma, dma((rounds, far)),
            dma, dma((rounds, groups - 1)), dma((2,)), dma, dma((groups - 1,)),
        ],
        compiler_params=pltpu.CompilerParams(
            collective_id=0, has_side_effects=True, vmem_limit_bytes=48 * 2**20
        ),
    )(order, sends, bag_rows, bag_lengths, weights, accum)


def body(grad_pooled, bag_rows, bag_lengths, table_order, weights, accum):
    held, row_count, width = weights.shape
    samples, tables, _ = grad_pooled.shape
    split = Split(lax.axis_size("group"), lax.axis_size("shard"))
    groups, lines, plane = split.groups, split.lines, split.plane
    quarter = held // groups
    batch = 2 if quarter % 32 == 0 else 1
    rounds = quarter // batch
    steps = lines * rounds
    offset = row_count // 2

    i, line, p, k = np.meshgrid(*map(np.arange, (rounds, lines, plane, batch)), indexing="ij")
    group, shard = split.device(i, p, line)
    slots = (shard * held + group * quarter + i * batch + k).reshape(-1)
    numbers = np.arange(tables)
    from_slot = jnp.asarray(slots[:, None] == numbers[None, :])
    order = jnp.sum(jnp.where(from_slot, table_order[None, :], 0), axis=1)
    at_slot = jnp.asarray(np.argsort(slots), jnp.int32)
    table_at = table_order[None, :] == jnp.arange(tables, dtype=jnp.int32)[:, None]
    places = jnp.sum(jnp.where(table_at, at_slot[None, :], 0), axis=1)

    sends = arrange(grad_pooled, places).reshape(steps, plane, batch, samples, width)
    new_weights, new_accum = exchange(
        order, sends, jnp.transpose(bag_rows, (0, 2, 1)), bag_lengths,
        weights.reshape(groups, quarter, row_count, width),
        accum.reshape(groups, quarter, row_count),
        split, offset,
    )
    return new_weights.reshape(weights.shape), new_accum.reshape(accum.shape)


def solution(mesh):
    in_specs = (
        P(AXES, None, None),
        P(AXES, None, None),
        P(AXES, None),
        P(),
        P("shard", None, None),
        P("shard", None),
    )
    out_specs = (P("shard", None, None), P("shard", None))
    return jax.shard_map(body, mesh=mesh, in_specs=in_specs, out_specs=out_specs, check_vma=False)
```
